32 devices in a mesh: group: 2 (over x), vocab: 16 (over z, y, core).
Axes of the slice: x: 2, y: 2, z: 4, core: 2. Of those that a mesh axis runs over, the one named last changes fastest.
Arguments:
- shard_ids: int32 [4096, 1], P(('group', 'vocab')), may hold values from 0 to 15; in each aligned block of 128 rows (0 to 127, 128 to 255, ...) at most 16 rows name the same one
- row_ids: int32 [4096], P(('group', 'vocab')), may hold values from 0 to 4007
- table: bfloat16 [64128, 4096], P('vocab', 'group'), may hold values from -6 to 6
- cotangent: bfloat16 [4096, 4096], P(('group', 'vocab')), may hold values from -6 to 6
Outputs:
- embeds: bfloat16 [4096, 4096], P(('group', 'vocab'))
- table_grad: bfloat16 [64128, 4096], P('vocab', 'group')
The draws below stay inside these ranges and needn't reach their ends.
Inputs may be any that keep to these rules, and one draw needn't show every extreme that they name: `shard_ids`: in each aligned block of 128 rows (the rows of one device), no shard is named by more than 16 rows, and in some blocks one shard is named by exactly 16.
All inputs are finite; a program needn't handle non-finite values.
Results may differ from the reference program's by a relative error of at most 0.001.
Values may be sent and summed in bfloat16 or wider, within the bound.
A program may use at most 128 MiB of HBM per device.

```python
import math
import jax
import jax.numpy as jnp
import numpy as np

D = 4096
V = 64128
TOK_DEV = 128
TOKENS = 4096
SHARD_ROWS = 4008
CAP = 16
N_VOCAB = 16


def plant(result, key, smallest, largest):
    dims = result.shape
    spot = [jax.random.randint(jax.random.fold_in(key, axis), (), 0, dims[axis]) for axis in range(len(dims))]
    result = result.at[tuple(spot)].set(smallest)
    longest = dims.index(max(dims))
    spot[longest] = (spot[longest] + 1) % dims[longest]
    return result.at[tuple(spot)].set(largest)


def block_scale(own_key, extent, shards, low, top_value):
    def one(axis_at, shards_of):
        draws = jax.random.uniform(jax.random.fold_in(jax.random.fold_in(own_key, 6), axis_at), (shards_of,), jnp.float32, low / len(shards), top_value / len(shards))
        return jnp.repeat(jnp.exp(draws), extent[axis_at] // shards_of).reshape((-1,) + (1,) * (len(extent) - axis_at - 1))

    level = one(*shards[0])
    for cut in shards[1:]:
        level = level * one(*cut)
    return level


def cumulative_ranks(amount, skew):
    loads = [(1 << 20) // math.isqrt(standing ** skew) + 1 for standing in range(1, amount + 1)]
    deviation = 1 + sum(loads) // (1 << 30)
    return np.cumsum(np.array([max(1, weight // deviation) for weight in loads]))


def ranked(stream_key, shape, number_of, slope):
    grid = cumulative_ranks(number_of, slope)
    pick = jax.random.randint(jax.random.fold_in(stream_key, 1), shape, 0, int(grid[number_of - 1]))
    grade = jnp.searchsorted(jnp.asarray(grid, jnp.int32), pick, side="right")
    return jax.random.permutation(jax.random.fold_in(stream_key, 2), number_of)[grade].astype(jnp.int32)


def shared_out(own_key, own, number, rows, amount, top, reach, skew):
    sequence = jax.random.permutation(own_key, amount)
    crowded, usual = shares(amount, rows * top, reach, skew, True), shares(amount, rows * top, reach, skew, False)
    places = jnp.arange(amount)

    def named(tallies, rotation):
        used = int((tallies > 0).sum())
        fixed = max(1, used // 4)
        moved = fixed + (places - fixed + rotation * (used - fixed)) % max(1, amount - fixed)
        return jnp.zeros((amount,), jnp.int32).at[sequence[jnp.where(places < fixed, places, moved)]].set(jnp.asarray(tallies, jnp.int32))

    tallies = jnp.where(number % 4 == 0, named(crowded, number // 4), named(usual, number - number // 4 - 1))
    mixed = jax.random.permutation(jax.random.fold_in(own, 3), amount)
    giver, sink = mixed[0:amount // 2 * 2:2], mixed[1:amount // 2 * 2:2]
    slack = jnp.minimum(tallies[giver] - 1, reach - tallies[sink]) // 2
    slack = jnp.where((giver == sequence[0]) | (sink == sequence[0]) | (tallies[sink] == 0), 0, jnp.maximum(slack, 0))
    moved = jax.random.randint(jax.random.fold_in(own, 4), (amount // 2,), 0, 1 << 20) % (slack + 1)
    tallies = tallies.at[giver].add(-moved).at[sink].add(moved)
    items = jnp.searchsorted(jnp.cumsum(tallies), jnp.arange(rows * top), side="right").astype(jnp.int32)
    listing = items.reshape(top, rows).T
    listing = listing[jax.random.permutation(jax.random.fold_in(own, 1), rows)]
    rotation = jax.random.randint(jax.random.fold_in(own, 2), (rows, 1), 0, top)
    return jnp.take_along_axis(listing, (jnp.arange(top)[None, :] + rotation) % top, axis=1)


def shares(count, total, bound, lean, full):
    weights = [(1 << 20) // math.isqrt(rank ** lean) + 1 for rank in range(1, count + 1)]
    largest = bound if full else min(bound, max(-(-total // count), total * weights[0] // sum(weights)))
    least = 1 if total - largest >= count - 1 else 0
    counts, spare = [largest] + [least] * (count - 1), total - largest - least * (count - 1)
    while spare > 0:
        free = [i for i in range(1, count) if counts[i] < largest] or [i for i in range(1, count) if counts[i] < bound]
        mass, budget = sum([weights[i] for i in free]), spare
        for i in free:
            more = min(bound - counts[i], max(1, budget * weights[i] // mass), spare)
            counts[i] = counts[i] + more
            spare = spare - more
    return np.array(counts)


def centred(stream_key, shape, spread, most, split=(), dtype=jnp.bfloat16):
    loudness = block_scale(stream_key, shape, split, -0.22, 0.18) if split else 1.0
    entries = jax.random.normal(stream_key, shape, jnp.float32) * spread * loudness
    return jnp.minimum(jnp.maximum(entries, -most), most).astype(dtype)


def setup_inputs(seed: int = 0) -> dict:
    splits = jax.random.split(jax.random.key(seed), 5)
    shard_ids_keys = jax.random.split(jax.random.fold_in(splits[0], 1), TOKENS // TOK_DEV)
    shard_ids_turns = jax.random.permutation(jax.random.fold_in(splits[0], 3), TOKENS // TOK_DEV)
    shard_ids = jax.vmap(lambda own, number: shared_out(jax.random.fold_in(splits[0], 2), own, number, TOK_DEV, N_VOCAB, 1, CAP, 2))(shard_ids_keys, shard_ids_turns).reshape((TOKENS, 1))
    row_ids = plant(ranked(splits[1], (TOKENS,), SHARD_ROWS, 2), jax.random.fold_in(splits[1], 3), 0, SHARD_ROWS - 1).astype(jnp.int32)
    table = centred(splits[2], (V, D), 1.0, 6.0, ((0, 16), (1, 2)))
    cotangent = centred(splits[3], (TOKENS, D), 1.0, 6.0, ((0, 32),))
    return {"shard_ids": shard_ids, "row_ids": row_ids, "table": table, "cotangent": cotangent}


def reference(shard_ids, row_ids, table, cotangent):
    token_ids = (shard_ids[:, 0] * (V // N_VOCAB) + row_ids).astype(jnp.int32)
    embeds = jnp.take(table, token_ids, axis=0)
    summed = jax.ops.segment_sum(cotangent.astype(jnp.float32), token_ids, num_segments=V)
    return embeds, summed.astype(jnp.bfloat16)
```

```python
import functools

import jax
import jax.numpy as jnp
from jax import lax
from jax.experimental import pallas as pl
from jax.experimental.pallas import tpu as pltpu
from jax.sharding import PartitionSpec as P

BOTH = ("group", "vocab")
PLANES = 4
CHUNKS = 8
EARLY = 32
LEVELS = (80, 96, 128)
F32 = jnp.float32
BF16 = jnp.bfloat16
I32 = jnp.int32
NT = (((1,), (1,)), ((), ()))


def direct(shard_ids, row_ids, table, cotangent):
    tokens, width = cotangent.shape
    groups = lax.axis_size("group")
    owners = lax.axis_size("vocab")
    per_owner = 2 * tokens // owners
    slots = owners * per_owner
    rows_here, cols = table.shape
    shard = shard_ids[:, 0]
    owner_hot = (shard[:, None] == jnp.arange(owners, dtype=I32)[None, :]).astype(BF16)
    earlier = jnp.tril(jnp.ones((tokens, tokens), BF16), -1)
    before = jnp.dot(earlier, owner_hot, preferred_element_type=F32)
    ranking = jnp.sum(before * owner_hot.astype(F32), axis=1).astype(I32)
    slot_index = shard * per_owner + ranking
    slot_hot = slot_index[:, None] == jnp.arange(slots, dtype=I32)[None, :]
    slot_mask = slot_hot.astype(BF16)
    outgoing = jnp.sum(jnp.where(slot_hot, (row_ids + 1)[:, None], 0), axis=0) - 1
    placed = jnp.concatenate(
        [
            lax.dot_general(
                slot_mask,
                cotangent[:, g * cols : (g + 1) * cols],
                (((0,), (0,)), ((), ())),
                preferred_element_type=F32,
            ).astype(BF16)
            for g in range(groups)
        ],
        axis=0,
    )
    arrived = lax.all_to_all(placed, BOTH, split_axis=0, concat_axis=0, tiled=True)
    asked = jnp.concatenate([outgoing] * groups)
    received = lax.all_to_all(asked, BOTH, split_axis=0, concat_axis=0, tiled=True)
    picker = (received[:, None] == jnp.arange(rows_here, dtype=I32)[None, :]).astype(BF16)
    found = jnp.dot(picker, table, preferred_element_type=F32).astype(BF16)
    homed = lax.all_to_all(found, BOTH, split_axis=0, concat_axis=0, tiled=True)
    table_grad = lax.dot_general(
        picker, arrived, (((0,), (0,)), ((), ())), preferred_element_type=F32
    ).astype(BF16)
    embeds = jnp.concatenate(
        [
            jnp.dot(
                slot_mask, homed[g * slots : (g + 1) * slots], preferred_element_type=F32
            ).astype(BF16)
            for g in range(groups)
        ],
        axis=1,
    )
    return embeds, table_grad


def exchange_kernel(
    early,
    late,
    per_line,
    ints,
    cot,
    table,
    embeds,
    arrived,
    rowslot_out,
    pick,
    tab,
    es,
    er,
    fs,
    ei,
    ls,
    lr,
    gs,
    ar,
    pg,
    pe,
    bo,
    be,
    bl,
    uo,
    ul,
    tab_sem,
    out_sem,
    es_s,
    es_r,
    ip_s,
    ip_r,
    ls_s,
    ls_r,
    gp_s,
    gp_r,
):
    groups = lax.axis_size("group")
    quads = lax.axis_size("vocab") // PLANES
    lines = groups * quads
    tokens = cot.shape[0]
    rows_here, cols = table.shape
    chunks, _, width, cw = ei.shape
    g = lax.axis_index("group")
    v = lax.axis_index("vocab")
    z = v // quads
    q = v % quads
    line = g * quads + q
    zs = (z, z + 1 - 2 * (z % 2), (z + 2) % PLANES, PLANES - 1 - z)
    early_at = (None, 0, early[0], early[0] + early[1])
    late_at = (None, 0, late[0], late[0] + late[1])

    def z_peer(k):
        return (g, zs[k] * quads + q)

    def line_peer(r):
        other = (line + r) % lines
        return other, (other // quads, z * quads + other % quads)

    def tab_copy(j, slot):
        return pltpu.make_async_copy(
            table.at[:, pl.ds(pl.multiple_of(j * cw, cw), cw)],
            tab.at[slot, pl.ds(0, rows_here), :],
            tab_sem.at[slot],
        )

    tab_copy(0, 0).start()
    barrier = pltpu.get_barrier_semaphore()
    for k in (1, 2, 3):
        pl.semaphore_signal(barrier, inc=1, device_id=z_peer(k), device_id_type=pl.DeviceIdType.MESH)
    for r in range(1, lines):
        pl.semaphore_signal(barrier, inc=1, device_id=line_peer(r)[1], device_id_type=pl.DeviceIdType.MESH)

    def meta(gg, zz, qq, i):
        return ints[i, pl.ds((gg * PLANES + zz) * quads + qq, 1), :]

    own = [meta(g, z, q, i) for i in range(5)]
    own_plane = own[0] // quads

    def hot(rows, index, valid):
        at = lax.broadcasted_iota(I32, (rows, tokens), 0)
        return jnp.where((at == index) & valid, 1.0, 0.0).astype(BF16)

    lane = lax.broadcasted_iota(I32, (1, tokens), 1)

    send_early = jnp.concatenate(
        [hot(early[k - 1], own[2], own_plane == zs[k]) for k in (1, 2, 3)], axis=0
    )
    step = 512
    for c in range(cot.shape[1] // step):
        es[:, c * step : (c + 1) * step] = jnp.dot(
            send_early, cot[:, c * step : (c + 1) * step], preferred_element_type=F32
        ).astype(BF16)

    pl.semaphore_wait(barrier, 3 + lines - 1)

    def early_copy(k):
        rows = pl.ds(early_at[k], early[k - 1])
        return pltpu.make_async_remote_copy(
            src_ref=es.at[rows, :],
            dst_ref=er.at[rows, :],
            send_sem=es_s.at[k - 1],
            recv_sem=es_r.at[k - 1],
            device_id=z_peer(k),
            device_id_type=pl.DeviceIdType.MESH,
        )

    for k in (2, 3, 1):
        early_copy(k).start()

    for other in range(lines):
        total = jnp.zeros((per_line, 1), I32)
        for zz in range(PLANES):
            gg, qq = other // quads, other % quads
            sh, row, rank = (meta(gg, zz, qq, i) for i in (0, 1, 3))
            at = lax.broadcasted_iota(I32, (per_line, tokens), 0)
            total += jnp.sum(
                jnp.where((at == rank) & (sh == v), row + 1, 0), axis=1, keepdims=True
            )
        asked = total - 1
        rowslot_out[other * per_line : (other + 1) * per_line, :] = jnp.broadcast_to(
            asked, (per_line, rowslot_out.shape[1])
        )
        wide = 512
        for c in range(pick.shape[1] // wide):
            at = lax.broadcasted_iota(I32, (per_line, wide), 1) + c * wide
            pick[other * per_line : (other + 1) * per_line, c * wide : (c + 1) * wide] = jnp.where(
                at == asked, 1.0, 0.0
            ).astype(BF16)
    if tab.shape[1] > rows_here:
        tab[:, rows_here:, :] = jnp.zeros((2, tab.shape[1] - rows_here, cw), BF16)

    def ip_copy(j, r):
        other, peer = line_peer(r)
        return pltpu.make_async_remote_copy(
            src_ref=fs.at[j, pl.ds(pl.multiple_of(other * per_line, per_line), per_line), :],
            dst_ref=ei.at[j, g, pl.ds(pl.multiple_of(q * per_line, per_line), per_line), :],
            send_sem=ip_s.at[j, r - 1],
            recv_sem=ip_r.at[j, r - 1],
            device_id=peer,
            device_id_type=pl.DeviceIdType.MESH,
        )

    @pl.loop(0, chunks)
    def _(j):
        slot = j % 2
        tab_copy(j, slot).wait()

        @pl.when(j + 1 < chunks)
        def _():
            tab_copy(j + 1, 1 - slot).start()

        fs[j] = jnp.dot(pick[...], tab[slot], preferred_element_type=F32).astype(BF16)
        mine = pl.ds(pl.multiple_of(line * per_line, per_line), per_line)
        ei[j, g, pl.ds(pl.multiple_of(q * per_line, per_line), per_line), :] = fs[j, mine, :]
        for r in range(1, lines):
            ip_copy(j, r).start()

    def count(device_row, plane):
        return jnp.sum(jnp.where(lane == plane, device_row, 0), axis=1, keepdims=True)

    def placed(rows, m):
        return (m[0] % quads) * per_line + m[3]

    slot_row = placed(width, own)
    here = own_plane == z
    bo[...] = hot(width, slot_row, here)
    back = [jnp.where(here, slot_row, -1)]
    for k in (1, 2, 3):
        m = [meta(g, zs[k], q, i) for i in range(5)]
        bound = (m[0] // quads) == z
        spill_out = jnp.maximum(count(own[4], zs[k]) - early[k - 1], 0)
        spill_in = jnp.maximum(count(m[4], z) - early[k - 1], 0)
        n = late[k - 1]
        to = own_plane == zs[k]
        at = late_at[k]
        slots = hot(width, placed(width, m), bound)
        pg[at : at + n, :] = hot(n, own[2] - early[k - 1], to & (own[2] >= early[k - 1]))
        pe[at : at + n, :] = lax.dot_general(
            hot(n, spill_out + m[2], bound), slots, NT, preferred_element_type=F32
        ).astype(BF16)
        be[:, early_at[k] : early_at[k] + early[k - 1]] = lax.dot_general(
            slots, hot(early[k - 1], m[2], bound), NT, preferred_element_type=F32
        ).astype(BF16)
        bl[:, at : at + n] = lax.dot_general(
            slots,
            hot(n, m[2] - early[k - 1], bound & (m[2] >= early[k - 1])),
            NT,
            preferred_element_type=F32,
        ).astype(BF16)
        back.append(jnp.where(to, at + spill_in + own[2], -1))
    merged = jnp.maximum(jnp.maximum(back[1], back[2]), back[3])
    stacked = jnp.concatenate([back[0], merged, jnp.zeros((6, tokens), I32)], axis=0).T
    uo[...] = jnp.where(
        lax.broadcasted_iota(I32, (tokens, width), 1) == stacked[:, 0:1], 1.0, 0.0
    ).astype(BF16)
    ul[...] = jnp.where(
        lax.broadcasted_iota(I32, ul.shape, 1) == stacked[:, 1:2], 1.0, 0.0
    ).astype(BF16)

    def late_copy(j, k):
        rows = pl.ds(late_at[k], late[k - 1])
        return pltpu.make_async_remote_copy(
            src_ref=ls.at[j, :, rows, :],
            dst_ref=lr.at[j, :, rows, :],
            send_sem=ls_s.at[j, k - 1],
            recv_sem=ls_r.at[j, k - 1],
            device_id=z_peer(k),
            device_id_type=pl.DeviceIdType.MESH,
        )

    def cot_cols(j, gg):
        return pl.ds(pl.multiple_of(gg * cols + j * cw, cw), cw)

    @pl.loop(0, chunks)
    def _(j):
        for r in range(1, lines):
            ip_copy(j, r).wait_recv()
        for gg in range(groups):
            ls[j, gg] = (
                jnp.dot(pg[...], cot[:, cot_cols(j, gg)], preferred_element_type=F32)
                + jnp.dot(pe[...], ei[j, gg], preferred_element_type=F32)
            ).astype(BF16)
        for k in (2, 3, 1):
            late_copy(j, k).start()

    for k in (1, 2, 3):
        early_copy(k).wait_recv()

    def gp_copy(j, r):
        other, peer = line_peer(r)
        return pltpu.make_async_remote_copy(
            src_ref=gs.at[
                j,
                other // quads,
                pl.ds(pl.multiple_of((other % quads) * per_line, per_line), per_line),
                :,
            ],
            dst_ref=ar.at[
                pl.ds(pl.multiple_of(line * per_line, per_line), per_line),
                pl.ds(pl.multiple_of(j * cw, cw), cw),
            ],
            send_sem=gp_s.at[j, r - 1],
            recv_sem=gp_r.at[j, r - 1],
            device_id=peer,
            device_id_type=pl.DeviceIdType.MESH,
        )

    @pl.loop(0, chunks)
    def _(j):
        for k in (1, 2, 3):
            late_copy(j, k).wait_recv()
        for gg in range(groups):
            gs[j, gg] = (
                jnp.dot(bo[...], cot[:, cot_cols(j, gg)], preferred_element_type=F32)
                + jnp.dot(be[...], er[:, cot_cols(j, gg)], preferred_element_type=F32)
                + jnp.dot(bl[...], lr[j, gg], preferred_element_type=F32)
            ).astype(BF16)
        for r in range(1, lines):
            gp_copy(j, r).start()
        ar[
            pl.ds(pl.multiple_of(line * per_line, per_line), per_line),
            pl.ds(pl.multiple_of(j * cw, cw), cw),
        ] = gs[j, g, pl.ds(pl.multiple_of(q * per_line, per_line), per_line), :]
        for gg in range(groups):
            embeds[:, cot_cols(j, gg)] = (
                jnp.dot(uo[...], ei[j, gg], preferred_element_type=F32)
                + jnp.dot(ul[...], lr[j, gg], preferred_element_type=F32)
            ).astype(BF16)

    def out_copy(j):
        part = pl.ds(pl.multiple_of(j * cw, cw), cw)
        return pltpu.make_async_copy(ar.at[:, part], arrived.at[:, part], out_sem.at[j])

    @pl.loop(0, chunks)
    def _(j):
        for r in range(1, lines):
            gp_copy(j, r).wait_recv()
        out_copy(j).start()

    for k in (1, 2, 3):
        early_copy(k).wait_send()

    @pl.loop(0, chunks)
    def _(j):
        for r in range(1, lines):
            ip_copy(j, r).wait_send()
            gp_copy(j, r).wait_send()
        for k in (1, 2, 3):
            late_copy(j, k).wait_send()
        out_copy(j).wait()


def exchange(level, ints, cot, table):
    tokens, width = cot.shape
    rows_here, cols = table.shape
    groups = lax.axis_size("group")
    shards = lax.axis_size("vocab")
    quads = shards // PLANES
    lines = groups * quads
    cap = 2 * tokens // shards
    per_line = PLANES * cap
    plane_cap = quads * cap
    block = LEVELS[level] * plane_cap // 64
    first = EARLY * plane_cap // 64
    early = (plane_cap, first, first)
    late = (plane_cap, block - first, block - first)
    cw = cols // CHUNKS
    slots = lines * per_line
    wide = quads * per_line
    deep = -(-rows_here // 512) * 512
    n_early, n_late = sum(early), sum(late)
    dma = pltpu.SemaphoreType.DMA
    return pl.pallas_call(
        functools.partial(exchange_kernel, early, late, per_line),
        out_shape=(
            jax.ShapeDtypeStruct((tokens, width), BF16),
            jax.ShapeDtypeStruct((slots, cols), BF16),
            jax.ShapeDtypeStruct((slots, 128), I32),
        ),
        in_specs=[
            pl.BlockSpec(memory_space=pltpu.VMEM),
            pl.BlockSpec(memory_space=pltpu.VMEM),
            pl.BlockSpec(memory_space=pl.ANY),
        ],
        out_specs=(
            pl.BlockSpec(memory_space=pltpu.VMEM),
            pl.BlockSpec(memory_space=pl.ANY),
            pl.BlockSpec(memory_space=pltpu.VMEM),
        ),
        scratch_shapes=[
            pltpu.VMEM((slots, deep), BF16),
            pltpu.VMEM((2, deep, cw), BF16),
            pltpu.VMEM((n_early, width), BF16),
            pltpu.VMEM((n_early, width), BF16),
            pltpu.VMEM((CHUNKS, slots, cw), BF16),
            pltpu.VMEM((CHUNKS, groups, wide, cw), BF16),
            pltpu.VMEM((CHUNKS, groups, n_late, cw), BF16),
            pltpu.VMEM((CHUNKS, groups, n_late, cw), BF16),
            pltpu.VMEM((CHUNKS, groups, wide, cw), BF16),
            pltpu.VMEM((slots, cols), BF16),
            pltpu.VMEM((n_late, tokens), BF16),
            pltpu.VMEM((n_late, wide), BF16),
            pltpu.VMEM((wide, tokens), BF16),
            pltpu.VMEM((wide, n_early), BF16),
            pltpu.VMEM((wide, n_late), BF16),
            pltpu.VMEM((tokens, wide), BF16),
            pltpu.VMEM((tokens, n_late), BF16),
            dma((2,)),
            dma((CHUNKS,)),
            dma((3,)),
            dma((3,)),
            dma((CHUNKS, lines - 1)),
            dma((CHUNKS, lines - 1)),
            dma((CHUNKS, 3)),
            dma((CHUNKS, 3)),
            dma((CHUNKS, lines - 1)),
            dma((CHUNKS, lines - 1)),
        ],
        compiler_params=pltpu.CompilerParams(
            collective_id=level, has_side_effects=True, vmem_limit_bytes=56 << 20
        ),
        name=f"exchange_{level}",
    )(ints, cot, table)


def index_kernel(plane_cap, blocks, shard, row, fields, level, mine, every, send, recv):
    groups = lax.axis_size("group")
    shards = lax.axis_size("vocab")
    quads = shards // PLANES
    devices = groups * shards
    tokens = shard.shape[0]
    me = lax.axis_index("group") * shards + lax.axis_index("vocab")

    def peer(r):
        other = (me + r) % devices
        return (other // shards, other % shards)

    barrier = pltpu.get_barrier_semaphore()
    for r in range(1, devices):
        pl.semaphore_signal(barrier, inc=1, device_id=peer(r), device_id_type=pl.DeviceIdType.MESH)

    down = jnp.broadcast_to(shard[...], (tokens, tokens))
    across = down.T
    lane = lax.broadcasted_iota(I32, (tokens, tokens), 1)
    earlier = lax.broadcasted_iota(I32, (tokens, tokens), 0) < lane

    def total(hits):
        return jnp.sum(jnp.where(hits, 1, 0), axis=0, keepdims=True)

    mine[...] = jnp.concatenate(
        [
            across[0:1, :],
            row[...],
            total((down // quads == across // quads) & earlier),
            total((down == across) & earlier),
            total(down // quads == lane),
            total(down == lane),
            jnp.zeros((2, tokens), I32),
        ],
        axis=0,
    )
    every[pl.ds(me, 1)] = mine[...][None]
    pl.semaphore_wait(barrier, devices - 1)

    def copy(r):
        return pltpu.make_async_remote_copy(
            src_ref=mine,
            dst_ref=every.at[me],
            send_sem=send.at[r - 1],
            recv_sem=recv.at[r - 1],
            device_id=peer(r),
            device_id_type=pl.DeviceIdType.MESH,
        )

    for r in range(1, devices):
        copy(r).start()
    for r in range(1, devices):
        copy(r).wait_recv()

    held = [every[:, i, :] for i in range(6)]
    i = lax.broadcasted_iota(I32, (devices, devices), 0)
    j = lax.broadcasted_iota(I32, (devices, devices), 1)
    ahead = (i // shards == j // shards) & (i % quads == j % quads) & (j < i)
    ahead = jnp.dot(
        jnp.where(ahead, 1.0, 0.0).astype(BF16), held[5].astype(F32).astype(BF16), preferred_element_type=F32
    ).astype(I32)
    rank = held[3]
    for s in range(shards):
        rank += jnp.where(held[0] == s, ahead[:, s : s + 1], 0)
    for f, value in enumerate((held[0], held[1], held[2], rank, held[4])):
        fields[f] = value
    first = EARLY * plane_cap // 64
    need = jnp.zeros((quads, 1), I32)
    half = PLANES // 2
    for g in range(groups):
        for p in range(half):
            for o in range(half, PLANES):
                at, to = g * shards + p * quads, g * shards + o * quads
                there = held[4][at : at + quads, o : o + 1]
                back = held[4][to : to + quads, p : p + 1]
                need = jnp.maximum(need, jnp.maximum(there, first) + back)
                need = jnp.maximum(need, jnp.maximum(back, first) + there)
    need = jnp.max(need)
    pick = jnp.zeros((), I32)
    for block in blocks[:-1]:
        pick += (need > block).astype(I32)
    level[0] = pick
    for r in range(1, devices):
        copy(r).wait_send()


def by_planes(shard_ids, row_ids, table, cotangent):
    tokens = cotangent.shape[0]
    devices = lax.axis_size("group") * lax.axis_size("vocab")
    plane_cap = 2 * tokens // PLANES
    blocks = tuple(b * plane_cap // 64 for b in LEVELS)
    dma = pltpu.SemaphoreType.DMA
    fields, level = pl.pallas_call(
        functools.partial(index_kernel, plane_cap, blocks),
        out_shape=(
            jax.ShapeDtypeStruct((5, devices, tokens), I32),
            jax.ShapeDtypeStruct((1,), I32),
        ),
        in_specs=[pl.BlockSpec(memory_space=pltpu.VMEM)] * 2,
        out_specs=(
            pl.BlockSpec(memory_space=pltpu.VMEM),
            pl.BlockSpec(memory_space=pltpu.SMEM),
        ),
        scratch_shapes=[
            pltpu.VMEM((8, tokens), I32),
            pltpu.VMEM((devices, 8, tokens), I32),
            dma((devices - 1,)),
            dma((devices - 1,)),
        ],
        compiler_params=pltpu.CompilerParams(collective_id=len(LEVELS), has_side_effects=True),
        name="indices",
    )(shard_ids, row_ids[None, :])
    embeds, arrived, asked = lax.switch(
        level[0],
        [functools.partial(exchange, i) for i in range(len(LEVELS))],
        fields,
        cotangent,
        table,
    )
    picker = (asked[:, :1] == jnp.arange(table.shape[0], dtype=I32)[None, :]).astype(BF16)
    table_grad = lax.dot_general(
        picker, arrived, (((0,), (0,)), ((), ())), preferred_element_type=F32
    ).astype(BF16)
    return embeds, table_grad


def solution(mesh):
    groups, shards = mesh.shape["group"], mesh.shape["vocab"]
    lines = shards == PLANES * PLANES and groups * shards == 2 * PLANES * PLANES
    in_specs = (
        P(BOTH, None),
        P(BOTH),
        P("vocab", "group"),
        P(BOTH, None),
    )
    out_specs = (P(BOTH, None), P("vocab", "group"))
    return jax.shard_map(
        by_planes if lines else direct,
        mesh=mesh,
        in_specs=in_specs,
        out_specs=out_specs,
        check_vma=False,
    )
```
